32 devices in a mesh: row: 8 (over z, y), col: 4 (over x, core).
Axes of the slice: x: 2, y: 2, z: 4, core: 2. Of those that a mesh axis runs over, the one named last changes fastest.
Arguments:
- spectrum: float32 [2, 4096, 2048], P(None, 'row', 'col'), may hold values from -6 to 6
- pupil: float32 [2, 512, 512], replicated, may hold values from -4.2 to 4.2
- amplitudes: float32 [8, 4, 1, 512, 512], P('row', 'col'), may hold values from 0.1 to 3
- offsets: int32 [8, 4, 1, 2], P('row', 'col'), may hold values from 0 to 511, as said below
- counts: int32 [8, 4], P('row', 'col'), may hold values from 1 to 1, as said below
Outputs:
- recovered: float32 [2, 4096, 2048], P(None, 'row', 'col')
The draws below stay inside these ranges and needn't reach their ends.
Inputs may be any that keep to these rules, and one draw needn't show every extreme that they name: `offsets`: offsets are corners inside the tile: the row below 512, the column below 512. `counts`: some device has all 1 slots live.
All inputs are finite; a program needn't handle non-finite values.
Results may differ from the reference program's by a relative error of at most 0.012.
Values sent between devices are 32-bit elements; how exact they have to be, the bound alone decides.
A program may use at most 128 MiB of HBM per device.

```python
import math
import jax
import jax.numpy as jnp
from jax import lax

W = 512
TR = 512
TC = 512
CAP = 1
SWEEPS = 2
NR = 4096
NC = 2048
N_ROW = 8
N_COL = 4


def draw_offsets(key, part):
    first = jax.random.randint(jax.random.fold_in(key, 11), (N_ROW, N_COL, CAP, 1), 0, TR)
    second = jax.random.randint(jax.random.fold_in(key, 12), (N_ROW, N_COL, CAP, 1), 0, TC)
    return jnp.concatenate([first, second], axis=3).astype(jnp.int32)


def draw_counts(key, part):
    base = jax.random.randint(jax.random.fold_in(key, 21), (N_ROW * N_COL,), 1, CAP + 1)
    chosen = jax.random.randint(jax.random.fold_in(key, 22), (), 0, N_ROW * N_COL)
    base = base.at[chosen].set(CAP)
    return base.reshape(N_ROW, N_COL).astype(jnp.int32)


def levels(own_key, dims, pieces, least, top_value):
    factor_of, own = 1.0, jax.random.fold_in(own_key, 6)
    for axis_at, blocks in pieces:
        draws = jnp.exp(jax.random.uniform(jax.random.fold_in(own, axis_at), (blocks,), jnp.float32, least / len(pieces), top_value / len(pieces)))
        factor_of = factor_of * jnp.repeat(draws, dims[axis_at] // blocks).reshape([-1 if axis == axis_at else 1 for axis in range(len(dims))])
    return factor_of


def normal_values(own_key, extent, scale, limit, shards=(), kind=jnp.bfloat16):
    drawn = scale * jax.random.normal(own_key, extent, jnp.float32)
    if shards:
        drawn = drawn * levels(own_key, extent, shards, -0.22, 0.18)
    return jnp.clip(drawn, -limit, limit).astype(kind)


def setup_inputs(seed: int = 0) -> dict:
    key_list = jax.random.split(jax.random.key(seed), 6)
    spectrum = normal_values(key_list[0], (2, NR, NC), 1.0, 6.0, ((1, 8), (2, 4)), jnp.float32)
    pupil = normal_values(key_list[1], (2, W, W), 0.7, 4.2, (), jnp.float32)
    amplitudes = jnp.clip(jnp.exp(math.log(3.0) - 3.4011974 * jax.random.uniform(key_list[2], (N_ROW, N_COL, CAP, W, W), jnp.float32) ** levels(key_list[2], (N_ROW, N_COL, CAP, W, W), ((0, 8), (1, 4)), -0.2, 0.2)), 0.1, 3.0)
    offsets = draw_offsets(jax.random.fold_in(key_list[5], 71), 0)
    counts = draw_counts(jax.random.fold_in(key_list[5], 71), 0)
    return {"spectrum": spectrum, "pupil": pupil, "amplitudes": amplitudes, "offsets": offsets, "counts": counts}


step_size = 0.5
floor_value = 0.05

def dft_tables(width):
    index = jnp.arange(width, dtype=jnp.int32)
    phase = index[:, None] * index[None, :] % width
    angle = phase.astype(jnp.float32) * (2.0 * math.pi / width)
    scale = 1.0 / math.sqrt(width)
    return ((jnp.cos(angle) * scale).astype(jnp.bfloat16), (jnp.sin(angle) * scale).astype(jnp.bfloat16))

def transform(real, imag, cosine, sine, sign):
    cosine = cosine.astype(jnp.float32)
    sine = sine.astype(jnp.float32)
    real = real.astype(jnp.bfloat16).astype(jnp.float32)
    imag = imag.astype(jnp.bfloat16).astype(jnp.float32)

    def right(a, b):
        return jnp.einsum('swk,kj->swj', a, b, precision=lax.Precision.HIGHEST)

    def left(b, a):
        return jnp.einsum('ik,skj->sij', b, a, precision=lax.Precision.HIGHEST)
    first_real = (right(real, cosine) - sign * right(imag, sine)).astype(jnp.bfloat16).astype(jnp.float32)
    first_imag = (right(imag, cosine) + sign * right(real, sine)).astype(jnp.bfloat16).astype(jnp.float32)
    out_real = left(cosine, first_real) - sign * left(sine, first_imag)
    out_imag = left(cosine, first_imag) + sign * left(sine, first_real)
    return (out_real, out_imag)

def slot_gradient(window_real, window_imag, pupil, amps, live, cosine, sine):
    pupil_real = pupil[0][None]
    pupil_imag = pupil[1][None]
    field_real = window_real * pupil_real - window_imag * pupil_imag
    field_imag = window_real * pupil_imag + window_imag * pupil_real
    wave_real, wave_imag = transform(field_real, field_imag, cosine, sine, 1.0)
    magnitude = jnp.sqrt(wave_real * wave_real + wave_imag * wave_imag)
    keep = 1.0 - amps / jnp.maximum(magnitude, floor_value)
    back_real, back_imag = transform(wave_real * keep, wave_imag * keep, cosine, sine, -1.0)
    mask = live[:, None, None]
    grad_real = (back_real * pupil_real + back_imag * pupil_imag) * mask
    grad_imag = (back_imag * pupil_real - back_real * pupil_imag) * mask
    return (grad_real, grad_imag)

def reference(spectrum, pupil, amplitudes, offsets, counts):
    cosine, sine = dft_tables(W)
    total_slots = N_ROW * N_COL * CAP
    flat_amps = amplitudes.reshape(total_slots, W, W)
    flat_offsets = offsets.reshape(total_slots, 2)
    flat_counts = counts.reshape(N_ROW * N_COL)
    for sweep in range(SWEEPS):
        padded = jnp.pad(spectrum, ((0, 0), (0, W), (0, W)))

        def one(index, total):
            device = index // CAP
            slot = index % CAP
            row_start = (device // N_COL * TR + flat_offsets[index, 0]).astype(jnp.int32)
            col_start = (device % N_COL * TC + flat_offsets[index, 1]).astype(jnp.int32)
            zero = jnp.zeros((), jnp.int32)
            window = lax.dynamic_slice(padded, (zero, row_start, col_start), (2, W, W))
            amp = lax.dynamic_slice_in_dim(flat_amps, index.astype(jnp.int32), 1, 0)
            live = (slot < flat_counts[device]).astype(jnp.float32)
            grad_real, grad_imag = slot_gradient(window[0][None], window[1][None], pupil, amp, live[None], cosine, sine)
            piece = jnp.stack([grad_real[0], grad_imag[0]])
            current = lax.dynamic_slice(total, (zero, row_start, col_start), (2, W, W))
            return lax.dynamic_update_slice(total, current + piece, (zero, row_start, col_start))
        total = lax.fori_loop(jnp.int32(0), jnp.int32(total_slots), one, jnp.zeros_like(padded))
        spectrum = spectrum - step_size * total[:, :NR, :NC]
    return spectrum
```

```python
import functools
import math

import jax
import jax.numpy as jnp
import numpy as np
from jax import lax
from jax.experimental import pallas as pl
from jax.experimental.pallas import tpu as pltpu
from jax.sharding import PartitionSpec as P

SWEEPS = 2
CHUNKS = 16
LAG = 3
RELAY = 2

step_size = 0.5
floor_value = 0.05

MESH = pl.DeviceIdType.MESH
BF16 = jnp.bfloat16
F32 = jnp.float32


def dft_tables(width):
    index = np.arange(width)
    angle = (index[:, None] * index[None, :] % width) * (2.0 * math.pi / width)
    scale = 1.0 / math.sqrt(width)
    return (
        jnp.asarray((np.cos(angle) * scale).astype(np.float32).astype(BF16)),
        jnp.asarray((np.sin(angle) * scale).astype(np.float32).astype(BF16)),
    )


def dot(a, b):
    return jnp.dot(a, b, preferred_element_type=F32)


def iota(shape, axis):
    return lax.broadcasted_iota(jnp.int32, shape, axis)


def kernel(
    n_row, n_col, place, count, spec, pupil_in, amps_in, cosine_in, sine_in, out,
    y1, z1, side1, mix1, win, grad1, from_left1, from_right1, give_p, got_p, give_z, got_z,
    total, from_left2, give_z2, got_z2, give_y2, got_y2,
    pup, fwd_right, fwd_left, back_right, back_left, f1, f2, hot,
    here, own, meta_l, meta_r, meta_p, meta_z,
    send, recv, meta_send, meta_recv, amps_sem,
    pupil, amps, cosine, sine, load,
):
    width = spec.shape[1]
    size = width // CHUNKS
    r, c = lax.axis_index("row"), lax.axis_index("col")
    parity = lax.rem(r, 2)
    mate = r + 1 - 2 * parity
    swapped = lax.rem(r // 2, 2) == 1
    home = jnp.where(swapped, mate, r)
    odd = lax.rem(home, 2) == 1
    even = jnp.logical_not(odd)
    has_z = jnp.where(odd, home < n_row - 1, home > 0)
    has_left, has_right = c > 0, c < n_col - 1
    left = (r, lax.rem(c + n_col - 1, n_col))
    right = (r, lax.rem(c + 1, n_col))
    partner = (mate, c)
    beyond = (lax.rem(jnp.where(odd, r + 2, r + n_row - 2), n_row), c)
    always = r >= 0
    side = jnp.where(odd, -1.0, 1.0)

    def both(*conditions):
        return functools.reduce(jnp.logical_and, conditions)

    def either(*conditions):
        return functools.reduce(jnp.logical_or, conditions)

    def when(condition, body):
        pl.when(condition)(body)

    stay = jnp.logical_not(swapped)
    loads = [
        pltpu.make_async_copy(source, target, load.at[at])
        for at, (source, target) in enumerate(
            ((cosine_in, cosine), (sine_in, sine), (pupil_in, pupil))
        )
    ]
    for copy in loads:
        copy.start()
    own_amps = pltpu.make_async_copy(amps_in, amps, load.at[3])
    when(stay, own_amps.start)
    for at, value in enumerate((place[0].astype(F32), place[1].astype(F32), jnp.where(count[0] > 0, 1.0, 0.0))):
        here[at] = jnp.zeros(here.shape[1:], F32) + value

    def ds(k, block=size, base=0):
        return pl.ds(pl.multiple_of(base + k * block, 8), block)

    def flow(kind, src, dst, device):
        def copy(k):
            return pltpu.make_async_remote_copy(
                src_ref=src.at[:, ds(k), :], dst_ref=dst.at[:, ds(k), :],
                send_sem=send.at[kind, k], recv_sem=recv.at[kind, k],
                device_id=device, device_id_type=MESH,
            )
        return copy

    def each(body, count=CHUNKS):
        def step(k, carry):
            body(k)
            return carry
        lax.fori_loop(0, count, step, 0)

    neighbours = ((always, partner), (has_z, beyond), (has_left, left), (has_right, right))
    barrier = pltpu.get_barrier_semaphore()
    for there, device in neighbours:
        @pl.when(there)
        def _():
            pl.semaphore_signal(barrier, inc=1, device_id=device, device_id_type=MESH)
    pl.semaphore_wait(barrier, sum(there.astype(jnp.int32) for there, _ in neighbours))

    def meta_copy(at, src, dst, device):
        return pltpu.make_async_remote_copy(
            src_ref=src, dst_ref=dst, send_sem=meta_send.at[at], recv_sem=meta_recv.at[at],
            device_id=device, device_id_type=MESH,
        )

    meta_swap = meta_copy(0, here, own, partner)
    meta_flows = (
        (meta_copy(1, own, meta_r, left), has_left, has_right),
        (meta_copy(2, own, meta_l, right), has_right, has_left),
        (meta_copy(3, own, meta_p, partner), always, always),
        (meta_copy(4, own, meta_z, beyond), has_z, has_z),
    )
    amps_flow = pltpu.make_async_remote_copy(
        src_ref=amps_in, dst_ref=amps, send_sem=amps_sem.at[0], recv_sem=amps_sem.at[1],
        device_id=partner, device_id_type=MESH,
    )

    y_in = (flow(0, spec, y1, partner), either(swapped, odd), either(swapped, even))
    z_from_spec = flow(1, spec, z1, beyond)
    z_from_y = flow(1, y1, z1, beyond)
    z_in = (z_from_spec, both(even, has_z), both(odd, has_z))
    mix_in = (flow(2, mix1, side1, left), has_left, has_right)
    grad_right = (flow(3, grad1, from_left1, right), has_right, has_left)
    grad_left = (flow(4, grad1, from_right1, left), has_left, has_right)
    over_p = (flow(5, give_p, got_p, partner), always, always)
    over_z = (flow(6, give_z, got_z, beyond), has_z, has_z)
    last_right = (flow(7, total, from_left2, right), has_right, has_left)
    z_out = (flow(8, give_z2, got_z2, beyond), both(odd, has_z), both(even, has_z))
    y_out = (flow(9, give_y2, got_y2, partner), either(swapped, even), either(swapped, odd))
    flows = (y_in, z_in, mix_in, grad_right, grad_left, over_p, over_z, last_right, z_out, y_out)

    def start(one, k):
        when(one[1], lambda: one[0](k).start())

    def arrive(one, k):
        when(one[2], lambda: one[0](k).wait_recv())

    when(swapped, meta_swap.start)

    def first_sends(k):
        start(y_in, k)
        when(both(stay, even, has_z), lambda: z_from_spec(k).start())

    each(first_sends)
    when(swapped, amps_flow.start)

    @pl.when(stay)
    def _():
        own[...] = here[...]

    def clear(*refs):
        for ref in refs:
            ref[...] = jnp.zeros_like(ref)

    when(jnp.logical_not(has_left), lambda: clear(from_left1, from_left2, meta_l))
    when(jnp.logical_not(has_right), lambda: clear(side1, from_right1, meta_r))
    when(jnp.logical_not(has_z), lambda: clear(z1, got_z, got_z2, meta_z))
    when(swapped, meta_swap.wait_recv)
    for copy, sends, _ in meta_flows:
        when(sends, copy.start)

    block = 128
    shape = (block, width)
    row_at, column_at, live = own[0, 0:1, :], own[1, 0:1, :], own[2, 0:1, :]

    def count_up(shape, axis):
        return iota(shape, axis).astype(F32)

    def wrapped(value):
        return jnp.where(value >= width, value - width, value)

    def one_hot(mask):
        return jnp.where(mask, 1.0, 0.0).astype(BF16)

    def columns_of(i):
        at = (iota(shape, 0) + i * block).astype(F32)
        hot[0, ds(i, block)] = one_hot(count_up(shape, 1) == wrapped(at + row_at))
        hot[1, ds(i, block)] = one_hot(count_up(shape, 1) == wrapped(at + column_at))

    each(columns_of, width // block)

    def rows_hot(i, shift):
        at = (iota(shape, 0) + i * block).astype(F32)
        return one_hot(at == wrapped(count_up(shape, 1) + shift))

    def tables(i):
        top, low = ds(i, block), ds(i, block, width)
        near, far = pl.ds(0, width), pl.ds(width, width)

        def put(ref, cos, sin, top_sign, low_sign):
            ref[top, near] = cos.astype(BF16)
            ref[low, far] = cos.astype(BF16)
            ref[top, far] = (top_sign * sin).astype(BF16)
            ref[low, near] = (low_sign * sin).astype(BF16)

        hot_rows = rows_hot(i, column_at)
        put(fwd_right, dot(hot_rows, cosine[...]), dot(hot_rows, sine[...]), 1.0, -1.0)
        hot_rows = rows_hot(i, row_at)
        put(back_left, dot(hot_rows, cosine[...]), dot(hot_rows, sine[...]), 1.0, -1.0)
        cos, sin = cosine[ds(i, block)], sine[ds(i, block)]
        put(fwd_left, dot(cos, hot[0]), dot(sin, hot[0]), -1.0, 1.0)
        put(back_right, dot(cos, hot[1]), dot(sin, hot[1]), -1.0, 1.0)

    for copy in loads:
        copy.wait()
    each(tables, width // block)

    def three(value):
        high = value.astype(BF16)
        rest = value - high.astype(F32)
        middle = rest.astype(BF16)
        return high, middle, (rest - middle.astype(F32)).astype(BF16)

    for plane in range(2):
        def pupil_columns(i):
            parts = three(pupil[plane, ds(i, block)])
            moved = [dot(part, hot[1]) for part in parts]
            f1[ds(i, block)] = moved[0].astype(BF16)
            f1[ds(i, block, width)] = moved[1].astype(BF16)
            f2[ds(i, block)] = moved[2].astype(BF16)

        each(pupil_columns, width // block)

        def pupil_rows(i):
            hot_rows = rows_hot(i, row_at)
            high = dot(hot_rows, f1[0:width])
            middle = dot(hot_rows, f1[width : 2 * width])
            pup[plane, ds(i, block)] = high + middle + dot(hot_rows, f2[0:width])

        each(pupil_rows, width // block)

    part = (size, width)

    def low_of(k, ref):
        return (iota(part, 0) + k * size).astype(F32) < ref[0, 0:1, :]

    def near_mate(k, ref):
        return side * ((iota(part, 0) + k * size).astype(F32) - ref[0, 0:1, :] + 0.5) < 0.0

    def far_of(ref):
        return count_up(part, 1) < ref[1, 0:1, :]

    def step_in(k, planes):
        rows = ds(k)
        pr, pi = pup[0, rows], pup[1, rows]
        field_real = planes[0] * pr - planes[1] * pi
        field_imag = planes[0] * pi + planes[1] * pr
        joined = jnp.concatenate([field_real, field_imag], axis=1).astype(BF16)
        first = dot(joined, fwd_right[...])
        f1[rows] = first[:, :width].astype(BF16)
        f1[ds(k, size, width)] = first[:, width:].astype(BF16)

    def tiles(k, p):
        rows = ds(k)
        near = jnp.where(swapped, y1[p, rows], spec[p, rows])
        mine = jnp.where(swapped, spec[p, rows], y1[p, rows])
        return near, jnp.where(odd, z1[p, rows], mine)

    def relay(k):
        arrive(y_in, k)
        when(both(swapped, even, has_z), lambda: z_from_y(k).start())

    def mix(k):
        arrive(z_in, k)
        rows = ds(k)
        own_low, left_low = low_of(k, own), low_of(k, meta_l)
        for p in range(2):
            near, below = tiles(k, p)
            win[p, rows] = jnp.where(own_low, below, near)
            mix1[p, rows] = jnp.where(left_low, below, near)
        start(mix_in, k)

    def consume(k):
        arrive(mix_in, k)
        rows, far = ds(k), far_of(own)
        planes = [jnp.where(far, side1[p, rows], win[p, rows]) for p in range(2)]
        for p in range(2):
            win[p, rows] = planes[p]
        step_in(k, planes)

    for copy, _, receives in meta_flows:
        when(receives, copy.wait_recv)

    relay(0)
    relay(1)
    mix(0)

    def gather(k):
        relay(k + 2)
        mix(k + 1)
        consume(k)

    each(gather, CHUNKS - 2)
    mix(CHUNKS - 1)
    consume(CHUNKS - 2)
    consume(CHUNKS - 1)

    wide = width // 2

    def middle(i):
        rows, low = ds(i, wide), ds(i, wide, width)
        wave = dot(jnp.concatenate([fwd_left[rows], fwd_left[low]], axis=0), f1[...])
        wave_real, wave_imag = wave[:wide], wave[wide:]
        magnitude = jnp.sqrt(wave_real * wave_real + wave_imag * wave_imag)
        keep = 1.0 - amps[rows] / jnp.maximum(magnitude, floor_value)
        joined = jnp.concatenate([wave_real * keep, wave_imag * keep], axis=1).astype(BF16)
        first = dot(joined, back_right[...])
        f2[rows] = first[:, :width].astype(BF16)
        f2[low] = first[:, width:].astype(BF16)

    def slope(k):
        rows, low = ds(k), ds(k, size, width)
        back = dot(jnp.concatenate([back_left[rows], back_left[low]], axis=0), f2[...])
        back_real, back_imag = back[:size], back[size:]
        pr, pi = pup[0, rows], pup[1, rows]
        return (
            (back_real * pr + back_imag * pi) * live,
            (back_imag * pr - back_real * pi) * live,
        )

    when(stay, own_amps.wait)
    when(swapped, amps_flow.wait_recv)
    each(middle, width // wide)

    def piece(k):
        rows = ds(k)
        grads = slope(k)
        for p in range(2):
            grad1[p, rows] = grads[p]
        start(grad_right, k)
        start(grad_left, k)

    def spread(k):
        arrive(grad_right, k)
        arrive(grad_left, k)
        rows = ds(k)
        mates, mates_l, mates_r = near_mate(k, own), near_mate(k, meta_l), near_mate(k, meta_r)
        far, far_l, far_r = far_of(own), far_of(meta_l), far_of(meta_r)
        far_p, far_z = far_of(meta_p), far_of(meta_z)
        for p in range(2):
            mine = grad1[p, rows]
            mine_near, mine_far = jnp.where(far, 0.0, mine), jnp.where(far, mine, 0.0)
            near = jnp.where(far_l, from_left1[p, rows], 0.0)
            past = jnp.where(far_r, 0.0, from_right1[p, rows])
            near_p, past_p = jnp.where(mates_l, near, 0.0), jnp.where(mates_r, past, 0.0)
            near_z, past_z = near - near_p, past - past_p
            give_p[p, rows] = jnp.where(
                far_p,
                jnp.where(mates, mine_far, 0.0) + past_p,
                jnp.where(mates, mine_near, 0.0) + near_p,
            )
            give_z[p, rows] = jnp.where(
                far_z,
                jnp.where(mates, 0.0, mine_far) + past_z,
                jnp.where(mates, 0.0, mine_near) + near_z,
            )
            beside = jnp.where(
                far, jnp.where(mates, past_p, past_z), jnp.where(mates, near_p, near_z)
            )
            win[p, rows] = win[p, rows] - step_size * (mine + beside)
        start(over_p, k)
        start(over_z, k)

    each(piece, LAG)

    def exchange(k):
        piece(k + LAG)
        spread(k)

    each(exchange, CHUNKS - LAG)
    each(lambda k: spread(k + CHUNKS - LAG), LAG)

    row_edge = jnp.where(both(odd, jnp.logical_not(has_z)), row_at, 0.0)
    column_edge = jnp.where(has_right, 0.0, column_at)

    def renew(k):
        arrive(over_p, k)
        arrive(over_z, k)
        rows, mates = ds(k), near_mate(k, own)
        inside = both(
            (iota(part, 0) + k * size).astype(F32) >= row_edge,
            count_up(part, 1) >= column_edge,
        )
        planes = [
            jnp.where(
                inside,
                win[p, rows] - step_size * jnp.where(mates, got_p[p, rows], got_z[p, rows]),
                0.0,
            )
            for p in range(2)
        ]
        step_in(k, planes)

    each(renew)
    each(middle, width // wide)

    def last_piece(k):
        rows = ds(k)
        grads = slope(k)
        for p in range(2):
            total[p, rows] = grad1[p, rows] + grads[p]
        start(last_right, k)

    def scatter(k):
        arrive(last_right, k)
        rows = ds(k)
        low, low_l, far, far_l = low_of(k, own), low_of(k, meta_l), far_of(own), far_of(meta_l)
        for p in range(2):
            mine = jnp.where(far, 0.0, total[p, rows])
            theirs = jnp.where(far_l, from_left2[p, rows], 0.0)
            mine_low, theirs_low = jnp.where(low, mine, 0.0), jnp.where(low_l, theirs, 0.0)
            lower = mine_low + theirs_low
            upper = (mine - mine_low) + (theirs - theirs_low)
            give_z2[p, rows] = lower
            give_y2[p, rows] = jnp.where(swapped, upper, lower)
            kept = jnp.where(swapped, jnp.where(odd, 0.0, lower), upper)
            out[p, rows] = spec[p, rows] - step_size * kept
        start(z_out, k)
        when(jnp.logical_not(both(swapped, even)), lambda: start(y_out, k))

    def pass_on(k):
        @pl.when(both(swapped, even))
        def _():
            arrive(z_out, k)
            rows = ds(k)
            for p in range(2):
                give_y2[p, rows] = give_y2[p, rows] + got_z2[p, rows]
            y_out[0](k).start()

    def finale(k):
        when(stay, lambda: arrive(z_out, k))
        arrive(y_out, k)
        rows = ds(k)
        for p in range(2):
            came = jnp.where(either(swapped, odd), got_y2[p, rows], got_z2[p, rows])
            out[p, rows] = out[p, rows] - step_size * came

    each(last_piece, LAG)

    def first_scatter(k):
        last_piece(k + LAG)
        scatter(k)

    each(first_scatter, RELAY)

    def steady(k):
        last_piece(k + LAG + RELAY)
        scatter(k + RELAY)
        pass_on(k)

    each(steady, CHUNKS - LAG - RELAY)

    def drain(k):
        scatter(k + CHUNKS - LAG)
        pass_on(k + CHUNKS - LAG - RELAY)

    each(drain, LAG)
    each(lambda k: pass_on(k + CHUNKS - RELAY), RELAY)
    each(finale)

    @pl.when(swapped)
    def _():
        meta_swap.wait_send()
        amps_flow.wait_send()

    for copy, sends, _ in meta_flows:
        when(sends, copy.wait_send)

    def sent(k):
        for one in flows:
            when(one[1], lambda: one[0](k).wait_send())

    each(sent)


def on_device(n_row, n_col, spectrum, pupil, amplitudes, offsets, counts):
    width = pupil.shape[1]
    amps = amplitudes[0, 0, 0]
    place = offsets.reshape(-1)
    count = counts.reshape(-1)
    cosine, sine = dft_tables(width)
    plane = pltpu.VMEM((2, width, width), F32)
    table = pltpu.VMEM((2 * width, 2 * width), BF16)
    stage = pltpu.VMEM((2 * width, width), BF16)
    note = pltpu.VMEM((3, 8, width), F32)
    vmem = pl.BlockSpec(memory_space=pltpu.VMEM)
    return pl.pallas_call(
        functools.partial(kernel, n_row, n_col),
        out_shape=jax.ShapeDtypeStruct(spectrum.shape, F32),
        in_specs=[pl.BlockSpec(memory_space=pltpu.SMEM)] * 2
        + [vmem]
        + [pl.BlockSpec(memory_space=pltpu.MemorySpace.HBM)] * 4,
        out_specs=vmem,
        scratch_shapes=[plane] * 19
        + [table] * 4
        + [stage] * 2
        + [pltpu.VMEM((2, width, width), BF16)]
        + [note] * 6
        + [
            pltpu.SemaphoreType.DMA((10, CHUNKS)),
            pltpu.SemaphoreType.DMA((10, CHUNKS)),
            pltpu.SemaphoreType.DMA((5,)),
            pltpu.SemaphoreType.DMA((5,)),
            pltpu.SemaphoreType.DMA((2,)),
            plane,
            pltpu.VMEM((width, width), F32),
            pltpu.VMEM((width, width), BF16),
            pltpu.VMEM((width, width), BF16),
            pltpu.SemaphoreType.DMA((4,)),
        ],
        compiler_params=pltpu.CompilerParams(
            collective_id=0, has_side_effects=True, vmem_limit_bytes=67 * 1000 * 1000
        ),
    )(place, count, spectrum, pupil, amps, cosine, sine)


def solution(mesh):
    in_specs = (
        P(None, "row", "col"),
        P(),
        P("row", "col", None, None, None),
        P("row", "col", None, None),
        P("row", "col"),
    )
    return jax.shard_map(
        functools.partial(on_device, mesh.shape["row"], mesh.shape["col"]),
        mesh=mesh, in_specs=in_specs, out_specs=P(None, "row", "col"), check_vma=False,
    )
```

```python
import functools
import math

import jax
import jax.numpy as jnp
import numpy as np
from jax import lax
from jax.experimental import pallas as pl
from jax.experimental.pallas import tpu as pltpu
from jax.sharding import PartitionSpec as P

SWEEPS = 2
CHUNKS = 16
DEPTH = 2
LAG = 3
BACK = 3
RELAY = 2

step_size = 0.5
floor_value = 0.05

MESH = pl.DeviceIdType.MESH
BF16 = jnp.bfloat16
F32 = jnp.float32


def dft_tables(width):
    index = np.arange(width)
    angle = (index[:, None] * index[None, :] % width) * (2.0 * math.pi / width)
    scale = 1.0 / math.sqrt(width)
    return (
        jnp.asarray((np.cos(angle) * scale).astype(np.float32).astype(BF16)),
        jnp.asarray((np.sin(angle) * scale).astype(np.float32).astype(BF16)),
    )


def dot(a, b):
    return jnp.dot(a, b, preferred_element_type=F32)


def iota(shape, axis):
    return lax.broadcasted_iota(jnp.int32, shape, axis)


def kernel(
    n_row, n_col, place, count, spec, pupil_in, amps_in, cosine_in, sine_in, out,
    y1, z1, side1, mix1, win, grad1, from_left1, from_right1, give_p, got_p, give_z, got_z,
    total, from_left2, give_z2, got_z2, give_y2, got_y2,
    pup, fwd_right, fwd_left, back_right, back_left, f1, f2, hot,
    here, own, meta_l, meta_r, meta_p, meta_z,
    send, recv, meta_send, meta_recv, amps_sem,
    pupil, amps, cosine, sine, load,
):
    width = spec.shape[1]
    size = width // CHUNKS
    r, c = lax.axis_index("row"), lax.axis_index("col")
    parity = lax.rem(r, 2)
    mate = r + 1 - 2 * parity
    swapped = lax.rem(r // 2, 2) == 1
    home = jnp.where(swapped, mate, r)
    odd = lax.rem(home, 2) == 1
    even = jnp.logical_not(odd)
    has_z = jnp.where(odd, home < n_row - 1, home > 0)
    has_left, has_right = c > 0, c < n_col - 1
    left = (r, lax.rem(c + n_col - 1, n_col))
    right = (r, lax.rem(c + 1, n_col))
    partner = (mate, c)
    beyond = (lax.rem(jnp.where(odd, r + 2, r + n_row - 2), n_row), c)
    always = r >= 0
    side = jnp.where(odd, -1.0, 1.0)

    def both(*conditions):
        return functools.reduce(jnp.logical_and, conditions)

    def either(*conditions):
        return functools.reduce(jnp.logical_or, conditions)

    def when(condition, body):
        if not isinstance(condition, bool):
            pl.when(condition)(body)
        elif condition:
            body()

    stay = jnp.logical_not(swapped)
    loads = [
        pltpu.make_async_copy(source, target, load.at[at])
        for at, (source, target) in enumerate(
            ((cosine_in, cosine), (sine_in, sine), (pupil_in, pupil))
        )
    ]
    for copy in loads:
        copy.start()
    own_amps = pltpu.make_async_copy(amps_in, amps, load.at[3])
    when(stay, own_amps.start)
    for at, value in enumerate((place[0].astype(F32), place[1].astype(F32), jnp.where(count[0] > 0, 1.0, 0.0))):
        here[at] = jnp.zeros(here.shape[1:], F32) + value

    def ds(k, block=size, base=0):
        return pl.ds(pl.multiple_of(base + k * block, 8), block)

    def flow(kind, src, dst, device):
        def copy(k):
            return pltpu.make_async_remote_copy(
                src_ref=src.at[:, ds(k), :], dst_ref=dst.at[:, ds(k), :],
                send_sem=send.at[kind, k], recv_sem=recv.at[kind, k],
                device_id=device, device_id_type=MESH,
            )
        return copy

    def each(body, count=CHUNKS):
        def step(k, carry):
            body(k)
            return carry
        lax.fori_loop(0, count, step, 0)

    neighbours = ((always, partner), (has_z, beyond), (has_left, left), (has_right, right))
    barrier = pltpu.get_barrier_semaphore()
    for there, device in neighbours:
        @pl.when(there)
        def _():
            pl.semaphore_signal(barrier, inc=1, device_id=device, device_id_type=MESH)
    pl.semaphore_wait(barrier, sum(there.astype(jnp.int32) for there, _ in neighbours))

    def meta_copy(at, src, dst, device):
        return pltpu.make_async_remote_copy(
            src_ref=src, dst_ref=dst, send_sem=meta_send.at[at], recv_sem=meta_recv.at[at],
            device_id=device, device_id_type=MESH,
        )

    meta_swap = meta_copy(0, here, own, partner)
    meta_flows = (
        (meta_copy(1, own, meta_r, left), has_left, has_right),
        (meta_copy(2, own, meta_l, right), has_right, has_left),
        (meta_copy(3, own, meta_p, partner), always, always),
        (meta_copy(4, own, meta_z, beyond), has_z, has_z),
    )
    amps_flow = pltpu.make_async_remote_copy(
        src_ref=amps_in, dst_ref=amps, send_sem=amps_sem.at[0], recv_sem=amps_sem.at[1],
        device_id=partner, device_id_type=MESH,
    )

    y_in = (flow(0, spec, y1, partner), either(swapped, odd), either(swapped, even))
    z_from_spec = flow(1, spec, z1, beyond)
    z_from_y = flow(1, y1, z1, beyond)
    z_in = (z_from_spec, both(even, has_z), both(odd, has_z))
    mix_in = (flow(2, mix1, side1, left), has_left, has_right)
    grad_right = (flow(3, grad1, from_left1, right), has_right, has_left)
    grad_left = (flow(4, grad1, from_right1, left), has_left, has_right)
    over_p = (flow(5, give_p, got_p, partner), always, always)
    over_z = (flow(6, give_z, got_z, beyond), has_z, has_z)
    last_right = (flow(7, total, from_left2, right), has_right, has_left)
    z_out = (flow(8, give_z2, got_z2, beyond), both(odd, has_z), both(even, has_z))
    y_out = (flow(9, give_y2, got_y2, partner), either(swapped, even), either(swapped, odd))
    flows = (y_in, z_in, mix_in, grad_right, grad_left, over_p, over_z, last_right, z_out, y_out)

    def launch(copy, k):
        when(k >= DEPTH, lambda: copy(k - DEPTH).wait_send())
        copy(k).start()

    def start(one, k):
        when(one[1], lambda: launch(one[0], k))

    def arrive(one, k):
        when(one[2], lambda: one[0](k).wait_recv())

    when(swapped, meta_swap.start)

    def first_sends(k):
        start(y_in, k)
        when(both(stay, even, has_z), lambda: launch(z_from_spec, k))

    for k in range(DEPTH):
        first_sends(k)

    @pl.when(stay)
    def _():
        own[...] = here[...]

    def clear(*refs):
        for ref in refs:
            ref[...] = jnp.zeros_like(ref)

    when(jnp.logical_not(has_left), lambda: clear(from_left1, from_left2, meta_l))
    when(jnp.logical_not(has_right), lambda: clear(side1, from_right1, meta_r))
    when(jnp.logical_not(has_z), lambda: clear(z1, got_z, got_z2, meta_z))
    when(swapped, meta_swap.wait_recv)
    for copy, sends, _ in meta_flows:
        when(sends, copy.start)

    row_at, column_at, live = own[0, 0:1, :], own[1, 0:1, :], own[2, 0:1, :]

    def count_up(shape, axis):
        return iota(shape, axis).astype(F32)

    part = (size, width)

    def low_of(k, ref):
        return (iota(part, 0) + k * size).astype(F32) < ref[0, 0:1, :]

    def near_mate(k, ref):
        return side * ((iota(part, 0) + k * size).astype(F32) - ref[0, 0:1, :] + 0.5) < 0.0

    def far_of(ref):
        return count_up(part, 1) < ref[1, 0:1, :]

    def tiles(k, p):
        rows = ds(k)
        near = jnp.where(swapped, y1[p, rows], spec[p, rows])
        mine = jnp.where(swapped, spec[p, rows], y1[p, rows])
        return near, jnp.where(odd, z1[p, rows], mine)

    def relay(k):
        arrive(y_in, k)
        when(both(swapped, even, has_z), lambda: launch(z_from_y, k))
        when(k + DEPTH < CHUNKS, lambda: first_sends(k + DEPTH))
        when(k + DEPTH == CHUNKS, lambda: when(swapped, amps_flow.start))

    def mix(k):
        arrive(z_in, k)
        rows = ds(k)
        own_low, left_low = low_of(k, own), low_of(k, meta_l)
        for p in range(2):
            near, below = tiles(k, p)
            win[p, rows] = jnp.where(own_low, below, near)
            mix1[p, rows] = jnp.where(left_low, below, near)
        start(mix_in, k)

    for copy, _, receives in meta_flows:
        when(receives, copy.wait_recv)

    def ahead(k):
        when(k + 2 < CHUNKS, lambda: relay(k + 2))
        mix(k)

    block = 128
    shape = (block, width)

    def wrapped(value):
        return jnp.where(value >= width, value - width, value)

    def one_hot(mask):
        return jnp.where(mask, 1.0, 0.0).astype(BF16)

    def columns_of(i):
        at = (iota(shape, 0) + i * block).astype(F32)
        hot[0, ds(i, block)] = one_hot(count_up(shape, 1) == wrapped(at + row_at))
        hot[1, ds(i, block)] = one_hot(count_up(shape, 1) == wrapped(at + column_at))

    each(columns_of, width // block)
    relay(0)
    relay(1)
    ahead(0)

    def rows_hot(i, shift):
        at = (iota(shape, 0) + i * block).astype(F32)
        return one_hot(at == wrapped(count_up(shape, 1) + shift))

    def tables(i):
        top, low = ds(i, block), ds(i, block, width)
        near, far = pl.ds(0, width), pl.ds(width, width)

        def put(ref, cos, sin, top_sign, low_sign):
            ref[top, near] = cos.astype(BF16)
            ref[low, far] = cos.astype(BF16)
            ref[top, far] = (top_sign * sin).astype(BF16)
            ref[low, near] = (low_sign * sin).astype(BF16)

        hot_rows = rows_hot(i, column_at)
        put(fwd_right, dot(hot_rows, cosine[...]), dot(hot_rows, sine[...]), 1.0, -1.0)
        hot_rows = rows_hot(i, row_at)
        put(back_left, dot(hot_rows, cosine[...]), dot(hot_rows, sine[...]), 1.0, -1.0)
        cos, sin = cosine[ds(i, block)], sine[ds(i, block)]
        put(fwd_left, dot(cos, hot[0]), dot(sin, hot[0]), -1.0, 1.0)
        put(back_right, dot(cos, hot[1]), dot(sin, hot[1]), -1.0, 1.0)

    for copy in loads:
        copy.wait()

    def beside(body, first, every):
        blocks = width // block

        def step(i):
            body(i)
            when(lax.rem(i, every) == every - 1, lambda: ahead(first + i // every))

        each(step, blocks)
        return first + blocks // every

    at = beside(tables, 1, 2)

    def three(value):
        high = value.astype(BF16)
        rest = value - high.astype(F32)
        middle = rest.astype(BF16)
        return high, middle, (rest - middle.astype(F32)).astype(BF16)

    for plane in range(2):
        def pupil_columns(i):
            parts = three(pupil[plane, ds(i, block)])
            moved = [dot(part, hot[1]) for part in parts]
            f1[ds(i, block)] = moved[0].astype(BF16)
            f1[ds(i, block, width)] = moved[1].astype(BF16)
            f2[ds(i, block)] = moved[2].astype(BF16)

        at = beside(pupil_columns, at, 4)

        def pupil_rows(i):
            hot_rows = rows_hot(i, row_at)
            high = dot(hot_rows, f1[0:width])
            middle = dot(hot_rows, f1[width : 2 * width])
            pup[plane, ds(i, block)] = high + middle + dot(hot_rows, f2[0:width])

        at = beside(pupil_rows, at, 4)

    def step_in(k, planes):
        rows = ds(k)
        pr, pi = pup[0, rows], pup[1, rows]
        field_real = planes[0] * pr - planes[1] * pi
        field_imag = planes[0] * pi + planes[1] * pr
        joined = jnp.concatenate([field_real, field_imag], axis=1).astype(BF16)
        first = dot(joined, fwd_right[...])
        f1[rows] = first[:, :width].astype(BF16)
        f1[ds(k, size, width)] = first[:, width:].astype(BF16)

    def consume(k):
        arrive(mix_in, k)
        rows, far = ds(k), far_of(own)
        planes = [jnp.where(far, side1[p, rows], win[p, rows]) for p in range(2)]
        for p in range(2):
            win[p, rows] = planes[p]
        step_in(k, planes)

    late = CHUNKS - at
    pairs = (CHUNKS - 2) - late

    def catch_up(k):
        ahead(at + k)
        consume(2 * k)
        consume(2 * k + 1)

    def keep_up(k):
        ahead(at + pairs + k)
        consume(2 * pairs + k)

    each(catch_up, pairs)
    each(keep_up, late - pairs)
    each(lambda k: consume(CHUNKS - 2 + k), 2)

    wide = width // 2

    def middle(i):
        rows, low = ds(i, wide), ds(i, wide, width)
        wave = dot(jnp.concatenate([fwd_left[rows], fwd_left[low]], axis=0), f1[...])
        wave_real, wave_imag = wave[:wide], wave[wide:]
        magnitude = jnp.sqrt(wave_real * wave_real + wave_imag * wave_imag)
        keep = 1.0 - amps[rows] / jnp.maximum(magnitude, floor_value)
        joined = jnp.concatenate([wave_real * keep, wave_imag * keep], axis=1).astype(BF16)
        first = dot(joined, back_right[...])
        f2[rows] = first[:, :width].astype(BF16)
        f2[low] = first[:, width:].astype(BF16)

    def slope(k):
        rows, low = ds(k), ds(k, size, width)
        back = dot(jnp.concatenate([back_left[rows], back_left[low]], axis=0), f2[...])
        back_real, back_imag = back[:size], back[size:]
        pr, pi = pup[0, rows], pup[1, rows]
        return (
            (back_real * pr + back_imag * pi) * live,
            (back_imag * pr - back_real * pi) * live,
        )

    when(stay, own_amps.wait)
    when(swapped, amps_flow.wait_recv)
    each(middle, width // wide)

    def piece(k):
        rows = ds(k)
        grads = slope(k)
        for p in range(2):
            grad1[p, rows] = grads[p]
        start(grad_right, k)
        start(grad_left, k)

    def spread(k):
        arrive(grad_right, k)
        arrive(grad_left, k)
        rows = ds(k)
        mates, mates_l, mates_r = near_mate(k, own), near_mate(k, meta_l), near_mate(k, meta_r)
        far, far_l, far_r = far_of(own), far_of(meta_l), far_of(meta_r)
        far_p, far_z = far_of(meta_p), far_of(meta_z)
        for p in range(2):
            mine = grad1[p, rows]
            mine_near, mine_far = jnp.where(far, 0.0, mine), jnp.where(far, mine, 0.0)
            near = jnp.where(far_l, from_left1[p, rows], 0.0)
            past = jnp.where(far_r, 0.0, from_right1[p, rows])
            near_p, past_p = jnp.where(mates_l, near, 0.0), jnp.where(mates_r, past, 0.0)
            near_z, past_z = near - near_p, past - past_p
            give_p[p, rows] = jnp.where(
                far_p,
                jnp.where(mates, mine_far, 0.0) + past_p,
                jnp.where(mates, mine_near, 0.0) + near_p,
            )
            give_z[p, rows] = jnp.where(
                far_z,
                jnp.where(mates, 0.0, mine_far) + past_z,
                jnp.where(mates, 0.0, mine_near) + near_z,
            )
            beside = jnp.where(
                far, jnp.where(mates, past_p, past_z), jnp.where(mates, near_p, near_z)
            )
            win[p, rows] = win[p, rows] - step_size * (mine + beside)
        start(over_p, k)
        start(over_z, k)

    each(piece, LAG)

    row_edge = jnp.where(both(odd, jnp.logical_not(has_z)), row_at, 0.0)
    column_edge = jnp.where(has_right, 0.0, column_at)

    def renew(k):
        arrive(over_p, k)
        arrive(over_z, k)
        rows, mates = ds(k), near_mate(k, own)
        inside = both(
            (iota(part, 0) + k * size).astype(F32) >= row_edge,
            count_up(part, 1) >= column_edge,
        )
        planes = [
            jnp.where(
                inside,
                win[p, rows] - step_size * jnp.where(mates, got_p[p, rows], got_z[p, rows]),
                0.0,
            )
            for p in range(2)
        ]
        step_in(k, planes)

    def exchange(k):
        when(k + LAG < CHUNKS, lambda: piece(k + LAG))
        spread(k)
        when(k >= BACK, lambda: renew(k - BACK))

    each(exchange)
    each(lambda k: renew(k + CHUNKS - BACK), BACK)
    each(middle, width // wide)

    def last_piece(k):
        rows = ds(k)
        grads = slope(k)
        for p in range(2):
            total[p, rows] = grad1[p, rows] + grads[p]
        start(last_right, k)

    def scatter(k):
        arrive(last_right, k)
        rows = ds(k)
        low, low_l, far, far_l = low_of(k, own), low_of(k, meta_l), far_of(own), far_of(meta_l)
        for p in range(2):
            mine = jnp.where(far, 0.0, total[p, rows])
            theirs = jnp.where(far_l, from_left2[p, rows], 0.0)
            mine_low, theirs_low = jnp.where(low, mine, 0.0), jnp.where(low_l, theirs, 0.0)
            lower = mine_low + theirs_low
            upper = (mine - mine_low) + (theirs - theirs_low)
            give_z2[p, rows] = lower
            give_y2[p, rows] = jnp.where(swapped, upper, lower)
            kept = jnp.where(swapped, jnp.where(odd, 0.0, lower), upper)
            out[p, rows] = spec[p, rows] - step_size * kept
        start(z_out, k)
        when(jnp.logical_not(both(swapped, even)), lambda: start(y_out, k))

    def pass_on(k):
        @pl.when(both(swapped, even))
        def _():
            arrive(z_out, k)
            rows = ds(k)
            for p in range(2):
                give_y2[p, rows] = give_y2[p, rows] + got_z2[p, rows]
            launch(y_out[0], k)

    def finale(k):
        when(stay, lambda: arrive(z_out, k))
        arrive(y_out, k)
        rows = ds(k)
        for p in range(2):
            came = jnp.where(either(swapped, odd), got_y2[p, rows], got_z2[p, rows])
            out[p, rows] = out[p, rows] - step_size * came

    each(last_piece, LAG)

    def first_scatter(k):
        last_piece(k + LAG)
        scatter(k)

    each(first_scatter, RELAY)

    def steady(k):
        last_piece(k + LAG + RELAY)
        scatter(k + RELAY)
        pass_on(k)

    each(steady, CHUNKS - LAG - RELAY)

    def drain(k):
        scatter(k + CHUNKS - LAG)
        pass_on(k + CHUNKS - LAG - RELAY)

    each(drain, LAG)
    each(lambda k: pass_on(k + CHUNKS - RELAY), RELAY)
    each(finale)

    @pl.when(swapped)
    def _():
        meta_swap.wait_send()
        amps_flow.wait_send()

    for copy, sends, _ in meta_flows:
        when(sends, copy.wait_send)

    def sent(k):
        for one in flows:
            when(one[1], lambda: one[0](k).wait_send())

    each(lambda k: sent(k + CHUNKS - DEPTH), DEPTH)


def on_device(n_row, n_col, spectrum, pupil, amplitudes, offsets, counts):
    width = pupil.shape[1]
    amps = amplitudes[0, 0, 0]
    place = offsets.reshape(-1)
    count = counts.reshape(-1)
    cosine, sine = dft_tables(width)
    plane = pltpu.VMEM((2, width, width), F32)
    table = pltpu.VMEM((2 * width, 2 * width), BF16)
    stage = pltpu.VMEM((2 * width, width), BF16)
    note = pltpu.VMEM((3, 8, width), F32)
    vmem = pl.BlockSpec(memory_space=pltpu.VMEM)
    return pl.pallas_call(
        functools.partial(kernel, n_row, n_col),
        out_shape=jax.ShapeDtypeStruct(spectrum.shape, F32),
        in_specs=[pl.BlockSpec(memory_space=pltpu.SMEM)] * 2
        + [vmem]
        + [pl.BlockSpec(memory_space=pltpu.MemorySpace.HBM)] * 4,
        out_specs=vmem,
        scratch_shapes=[plane] * 19
        + [table] * 4
        + [stage] * 2
        + [pltpu.VMEM((2, width, width), BF16)]
        + [note] * 6
        + [
            pltpu.SemaphoreType.DMA((10, CHUNKS)),
            pltpu.SemaphoreType.DMA((10, CHUNKS)),
            pltpu.SemaphoreType.DMA((5,)),
            pltpu.SemaphoreType.DMA((5,)),
            pltpu.SemaphoreType.DMA((2,)),
            plane,
            pltpu.VMEM((width, width), F32),
            pltpu.VMEM((width, width), BF16),
            pltpu.VMEM((width, width), BF16),
            pltpu.SemaphoreType.DMA((4,)),
        ],
        compiler_params=pltpu.CompilerParams(
            collective_id=0, has_side_effects=True, vmem_limit_bytes=67 * 1000 * 1000
        ),
    )(place, count, spectrum, pupil, amps, cosine, sine)


def solution(mesh):
    in_specs = (
        P(None, "row", "col"),
        P(),
        P("row", "col", None, None, None),
        P("row", "col", None, None),
        P("row", "col"),
    )
    return jax.shard_map(
        functools.partial(on_device, mesh.shape["row"], mesh.shape["col"]),
        mesh=mesh, in_specs=in_specs, out_specs=P(None, "row", "col"), check_vma=False,
    )
```

```python
import functools
import math

import jax
import jax.numpy as jnp
import numpy as np
from jax import lax
from jax.experimental import pallas as pl
from jax.experimental.pallas import tpu as pltpu
from jax.sharding import PartitionSpec as P

SWEEPS = 2
CHUNKS = 16
DEPTH = 2
LAG = 3
BACK = 3
RELAY = 2

step_size = 0.5
floor_value = 0.05

MESH = pl.DeviceIdType.MESH
BF16 = jnp.bfloat16
F32 = jnp.float32


def dft_tables(width):
    index = np.arange(width)
    angle = (index[:, None] * index[None, :] % width) * (2.0 * math.pi / width)
    scale = 1.0 / math.sqrt(width)
    return (
        jnp.asarray((np.cos(angle) * scale).astype(np.float32).astype(BF16)),
        jnp.asarray((np.sin(angle) * scale).astype(np.float32).astype(BF16)),
    )


def dot(a, b):
    return jnp.dot(a, b, preferred_element_type=F32)


def iota(shape, axis):
    return lax.broadcasted_iota(jnp.int32, shape, axis)


def kernel(
    n_row, n_col, place, count, spec, pupil_in, amps_in, cosine_in, sine_in, out,
    y1, z1, side1, mix1, win, grad1, from_left1, from_right1, give_p, got_p, give_z, got_z,
    total, from_left2, give_z2, got_z2, give_y2, got_y2,
    hop, pup, fwd_right, fwd_left, back_right, back_left, f1, f2, hot,
    here, own, meta_l, meta_r, meta_p, meta_z,
    send, recv, meta_send, meta_recv, amps_sem, first_amps, next_amps,
    pupil, amps, cosine, sine, load,
):
    width = spec.shape[1]
    size = width // CHUNKS
    r, c = lax.axis_index("row"), lax.axis_index("col")
    parity = lax.rem(r, 2)
    mate = r + 1 - 2 * parity
    swapped = lax.rem(r // 2, 2) == 1
    home = jnp.where(swapped, mate, r)
    odd = lax.rem(home, 2) == 1
    even = jnp.logical_not(odd)
    has_z = jnp.where(odd, home < n_row - 1, home > 0)
    has_left, has_right = c > 0, c < n_col - 1
    left = (r, lax.rem(c + n_col - 1, n_col))
    right = (r, lax.rem(c + 1, n_col))
    partner = (mate, c)
    beyond = (lax.rem(jnp.where(odd, r + 2, r + n_row - 2), n_row), c)
    has_cross = jnp.where(swapped, True, r + 2 < n_row)
    cross = (lax.rem(jnp.where(swapped, r + n_row - 2, r + 2), n_row), c)
    detour = lax.rem(c, 2) == 1
    always = r >= 0
    side = jnp.where(odd, -1.0, 1.0)

    def both(*conditions):
        return functools.reduce(jnp.logical_and, conditions)

    def either(*conditions):
        return functools.reduce(jnp.logical_or, conditions)

    def when(condition, body):
        if not isinstance(condition, bool):
            pl.when(condition)(body)
        elif condition:
            body()

    stay = jnp.logical_not(swapped)
    loads = [
        pltpu.make_async_copy(source, target, load.at[at])
        for at, (source, target) in enumerate(
            ((cosine_in, cosine), (sine_in, sine), (pupil_in, pupil))
        )
    ]
    for copy in loads:
        copy.start()
    own_amps = pltpu.make_async_copy(amps_in, amps, load.at[3])
    when(stay, own_amps.start)
    for at, value in enumerate((place[0].astype(F32), place[1].astype(F32), jnp.where(count[0] > 0, 1.0, 0.0))):
        here[at] = jnp.zeros(here.shape[1:], F32) + value

    def ds(k, block=size, base=0):
        return pl.ds(pl.multiple_of(base + k * block, 8), block)

    def flow(kind, src, dst, device):
        def copy(k):
            return pltpu.make_async_remote_copy(
                src_ref=src.at[:, ds(k), :], dst_ref=dst.at[:, ds(k), :],
                send_sem=send.at[kind, k], recv_sem=recv.at[kind, k],
                device_id=device, device_id_type=MESH,
            )
        return copy

    def flat(kind, src, dst, device):
        def copy(k):
            return pltpu.make_async_remote_copy(
                src_ref=src.at[ds(k), :], dst_ref=dst.at[ds(k), :],
                send_sem=send.at[kind, k], recv_sem=recv.at[kind, k],
                device_id=device, device_id_type=MESH,
            )
        return copy

    def each(body, count=CHUNKS):
        def step(k, carry):
            body(k)
            return carry
        lax.fori_loop(0, count, step, 0)

    neighbours = (
        (always, partner), (has_z, beyond), (has_left, left), (has_right, right),
        (both(parity == 0, has_cross), cross),
    )
    barrier = pltpu.get_barrier_semaphore()
    for there, device in neighbours:
        @pl.when(there)
        def _():
            pl.semaphore_signal(barrier, inc=1, device_id=device, device_id_type=MESH)
    pl.semaphore_wait(barrier, sum(there.astype(jnp.int32) for there, _ in neighbours))

    def meta_copy(at, src, dst, device):
        return pltpu.make_async_remote_copy(
            src_ref=src, dst_ref=dst, send_sem=meta_send.at[at], recv_sem=meta_recv.at[at],
            device_id=device, device_id_type=MESH,
        )

    meta_swap = meta_copy(0, here, own, partner)
    meta_flows = (
        (meta_copy(1, own, meta_r, left), has_left, has_right),
        (meta_copy(2, own, meta_l, right), has_right, has_left),
        (meta_copy(3, own, meta_p, partner), always, always),
        (meta_copy(4, own, meta_z, beyond), has_z, has_z),
    )

    y_in = (flow(0, spec, y1, partner), either(swapped, odd), either(swapped, even))
    direct = jnp.logical_not(detour)
    z_in = (
        flow(1, spec, z1, beyond), both(stay, even, has_z), both(odd, has_z, either(swapped, direct))
    )
    z_relay = (flow(1, y1, z1, beyond), both(swapped, even, has_z, direct), False)
    hop_in = (flow(10, spec, hop, cross), both(swapped, odd, detour), both(stay, even, has_cross, detour))
    z_hop = (flow(11, hop, z1, partner), both(stay, even, has_cross, detour), both(stay, odd, has_z, detour))
    relays_amps = both(stay, detour, has_cross)
    amps_1 = (flat(12, amps_in, first_amps, cross), both(swapped, detour), relays_amps)
    amps_2 = (flat(13, first_amps, next_amps, partner), relays_amps, relays_amps)
    amps_3 = (flat(14, next_amps, amps, cross), relays_amps, both(swapped, detour))
    straight = both(swapped, direct)
    amps_flow = pltpu.make_async_remote_copy(
        src_ref=amps_in, dst_ref=amps, send_sem=amps_sem.at[0], recv_sem=amps_sem.at[1],
        device_id=partner, device_id_type=MESH,
    )
    mix_in = (flow(2, mix1, side1, left), has_left, has_right)
    grad_right = (flow(3, grad1, from_left1, right), has_right, has_left)
    grad_left = (flow(4, grad1, from_right1, left), has_left, has_right)
    over_p = (flow(5, give_p, got_p, partner), always, always)
    over_z = (flow(6, give_z, got_z, beyond), has_z, has_z)
    last_right = (flow(7, total, from_left2, right), has_right, has_left)
    z_out = (flow(8, give_z2, got_z2, beyond), both(odd, has_z), both(even, has_z))
    y_out = (flow(9, give_y2, got_y2, partner), either(swapped, even), either(swapped, odd))
    flows = (y_in, z_in, mix_in, grad_right, grad_left, over_p, over_z, last_right, z_out, y_out,
             z_relay, hop_in, z_hop, amps_1, amps_2, amps_3)

    def launch(copy, k):
        when(k >= DEPTH, lambda: copy(k - DEPTH).wait_send())
        copy(k).start()

    def start(one, k):
        when(one[1], lambda: launch(one[0], k))

    def arrive(one, k):
        when(one[2], lambda: one[0](k).wait_recv())

    when(swapped, meta_swap.start)

    def first_sends(k):
        for one in (y_in, z_in, hop_in):
            start(one, k)

    for k in range(DEPTH):
        first_sends(k)
    for k in range(DEPTH):
        start(amps_1, k)

    @pl.when(stay)
    def _():
        own[...] = here[...]

    def clear(*refs):
        for ref in refs:
            ref[...] = jnp.zeros_like(ref)

    when(jnp.logical_not(has_left), lambda: clear(from_left1, from_left2, meta_l))
    when(jnp.logical_not(has_right), lambda: clear(side1, from_right1, meta_r))
    when(jnp.logical_not(has_z), lambda: clear(z1, got_z, got_z2, meta_z))
    when(swapped, meta_swap.wait_recv)
    for copy, sends, _ in meta_flows:
        when(sends, copy.start)

    row_at, column_at, live = own[0, 0:1, :], own[1, 0:1, :], own[2, 0:1, :]

    def count_up(shape, axis):
        return iota(shape, axis).astype(F32)

    part = (size, width)

    def low_of(k, ref):
        return (iota(part, 0) + k * size).astype(F32) < ref[0, 0:1, :]

    def near_mate(k, ref):
        return side * ((iota(part, 0) + k * size).astype(F32) - ref[0, 0:1, :] + 0.5) < 0.0

    def far_of(ref):
        return count_up(part, 1) < ref[1, 0:1, :]

    def tiles(k, p):
        rows = ds(k)
        near = jnp.where(swapped, y1[p, rows], spec[p, rows])
        mine = jnp.where(swapped, spec[p, rows], y1[p, rows])
        return near, jnp.where(odd, z1[p, rows], mine)

    def relay(k):
        arrive(y_in, k)
        start(z_relay, k)
        arrive(hop_in, k)
        start(z_hop, k)
        when(k + DEPTH < CHUNKS, lambda: first_sends(k + DEPTH))

    def mix(k):
        arrive(z_in, k)
        arrive(z_hop, k)
        rows = ds(k)
        own_low, left_low = low_of(k, own), low_of(k, meta_l)
        for p in range(2):
            near, below = tiles(k, p)
            win[p, rows] = jnp.where(own_low, below, near)
            mix1[p, rows] = jnp.where(left_low, below, near)
        start(mix_in, k)

    for copy, _, receives in meta_flows:
        when(receives, copy.wait_recv)

    def second(k):
        arrive(amps_1, k)
        start(amps_2, k)

    def third(k):
        arrive(amps_2, k)
        start(amps_3, k)

    def ahead(k):
        when(k + 2 < CHUNKS, lambda: relay(k + 2))
        mix(k)
        when(k + 4 < CHUNKS, lambda: start(amps_1, k + 4))
        when(k + 2 < CHUNKS, lambda: second(k + 2))
        third(k)
        when(k == CHUNKS - 2, lambda: when(straight, amps_flow.start))

    block = 128
    shape = (block, width)

    def wrapped(value):
        return jnp.where(value >= width, value - width, value)

    def one_hot(mask):
        return jnp.where(mask, 1.0, 0.0).astype(BF16)

    def columns_of(i):
        at = (iota(shape, 0) + i * block).astype(F32)
        hot[0, ds(i, block)] = one_hot(count_up(shape, 1) == wrapped(at + row_at))
        hot[1, ds(i, block)] = one_hot(count_up(shape, 1) == wrapped(at + column_at))

    each(columns_of, width // block)
    relay(0)
    relay(1)
    for k in range(DEPTH, 4):
        start(amps_1, k)
    second(0)
    second(1)
    ahead(0)

    def rows_hot(i, shift):
        at = (iota(shape, 0) + i * block).astype(F32)
        return one_hot(at == wrapped(count_up(shape, 1) + shift))

    def tables(i):
        top, low = ds(i, block), ds(i, block, width)
        near, far = pl.ds(0, width), pl.ds(width, width)

        def put(ref, cos, sin, top_sign, low_sign):
            ref[top, near] = cos.astype(BF16)
            ref[low, far] = cos.astype(BF16)
            ref[top, far] = (top_sign * sin).astype(BF16)
            ref[low, near] = (low_sign * sin).astype(BF16)

        hot_rows = rows_hot(i, column_at)
        put(fwd_right, dot(hot_rows, cosine[...]), dot(hot_rows, sine[...]), 1.0, -1.0)
        hot_rows = rows_hot(i, row_at)
        put(back_left, dot(hot_rows, cosine[...]), dot(hot_rows, sine[...]), 1.0, -1.0)
        cos, sin = cosine[ds(i, block)], sine[ds(i, block)]
        put(fwd_left, dot(cos, hot[0]), dot(sin, hot[0]), -1.0, 1.0)
        put(back_right, dot(cos, hot[1]), dot(sin, hot[1]), -1.0, 1.0)

    for copy in loads:
        copy.wait()

    def beside(body, first, every):
        blocks = width // block

        def step(i):
            body(i)
            when(lax.rem(i, every) == every - 1, lambda: ahead(first + i // every))

        each(step, blocks)
        return first + blocks // every

    at = beside(tables, 1, 2)

    def three(value):
        high = value.astype(BF16)
        rest = value - high.astype(F32)
        middle = rest.astype(BF16)
        return high, middle, (rest - middle.astype(F32)).astype(BF16)

    for plane in range(2):
        def pupil_columns(i):
            parts = three(pupil[plane, ds(i, block)])
            moved = [dot(part, hot[1]) for part in parts]
            f1[ds(i, block)] = moved[0].astype(BF16)
            f1[ds(i, block, width)] = moved[1].astype(BF16)
            f2[ds(i, block)] = moved[2].astype(BF16)

        at = beside(pupil_columns, at, 4)

        def pupil_rows(i):
            hot_rows = rows_hot(i, row_at)
            high = dot(hot_rows, f1[0:width])
            middle = dot(hot_rows, f1[width : 2 * width])
            pup[plane, ds(i, block)] = high + middle + dot(hot_rows, f2[0:width])

        at = beside(pupil_rows, at, 4)

    def step_in(k, planes):
        rows = ds(k)
        pr, pi = pup[0, rows], pup[1, rows]
        field_real = planes[0] * pr - planes[1] * pi
        field_imag = planes[0] * pi + planes[1] * pr
        joined = jnp.concatenate([field_real, field_imag], axis=1).astype(BF16)
        first = dot(joined, fwd_right[...])
        f1[rows] = first[:, :width].astype(BF16)
        f1[ds(k, size, width)] = first[:, width:].astype(BF16)

    def consume(k):
        arrive(mix_in, k)
        rows, far = ds(k), far_of(own)
        planes = [jnp.where(far, side1[p, rows], win[p, rows]) for p in range(2)]
        for p in range(2):
            win[p, rows] = planes[p]
        step_in(k, planes)

    late = CHUNKS - at
    pairs = (CHUNKS - 2) - late

    def catch_up(k):
        ahead(at + k)
        consume(2 * k)
        consume(2 * k + 1)

    def keep_up(k):
        ahead(at + pairs + k)
        consume(2 * pairs + k)

    each(catch_up, pairs)
    each(keep_up, late - pairs)
    each(lambda k: consume(CHUNKS - 2 + k), 2)

    wide = width // 2

    def middle(i):
        rows, low = ds(i, wide), ds(i, wide, width)
        wave = dot(jnp.concatenate([fwd_left[rows], fwd_left[low]], axis=0), f1[...])
        wave_real, wave_imag = wave[:wide], wave[wide:]
        magnitude = jnp.sqrt(wave_real * wave_real + wave_imag * wave_imag)
        keep = 1.0 - amps[rows] / jnp.maximum(magnitude, floor_value)
        joined = jnp.concatenate([wave_real * keep, wave_imag * keep], axis=1).astype(BF16)
        first = dot(joined, back_right[...])
        f2[rows] = first[:, :width].astype(BF16)
        f2[low] = first[:, width:].astype(BF16)

    def slope(k):
        rows, low = ds(k), ds(k, size, width)
        back = dot(jnp.concatenate([back_left[rows], back_left[low]], axis=0), f2[...])
        back_real, back_imag = back[:size], back[size:]
        pr, pi = pup[0, rows], pup[1, rows]
        return (
            (back_real * pr + back_imag * pi) * live,
            (back_imag * pr - back_real * pi) * live,
        )

    when(stay, own_amps.wait)

    each(lambda k: arrive(amps_3, k))
    when(straight, amps_flow.wait_recv)
    each(middle, width // wide)

    def piece(k):
        rows = ds(k)
        grads = slope(k)
        for p in range(2):
            grad1[p, rows] = grads[p]
        start(grad_right, k)
        start(grad_left, k)

    def spread(k):
        arrive(grad_right, k)
        arrive(grad_left, k)
        rows = ds(k)
        mates, mates_l, mates_r = near_mate(k, own), near_mate(k, meta_l), near_mate(k, meta_r)
        far, far_l, far_r = far_of(own), far_of(meta_l), far_of(meta_r)
        far_p, far_z = far_of(meta_p), far_of(meta_z)
        for p in range(2):
            mine = grad1[p, rows]
            mine_near, mine_far = jnp.where(far, 0.0, mine), jnp.where(far, mine, 0.0)
            near = jnp.where(far_l, from_left1[p, rows], 0.0)
            past = jnp.where(far_r, 0.0, from_right1[p, rows])
            near_p, past_p = jnp.where(mates_l, near, 0.0), jnp.where(mates_r, past, 0.0)
            near_z, past_z = near - near_p, past - past_p
            give_p[p, rows] = jnp.where(
                far_p,
                jnp.where(mates, mine_far, 0.0) + past_p,
                jnp.where(mates, mine_near, 0.0) + near_p,
            )
            give_z[p, rows] = jnp.where(
                far_z,
                jnp.where(mates, 0.0, mine_far) + past_z,
                jnp.where(mates, 0.0, mine_near) + near_z,
            )
            beside = jnp.where(
                far, jnp.where(mates, past_p, past_z), jnp.where(mates, near_p, near_z)
            )
            win[p, rows] = win[p, rows] - step_size * (mine + beside)
        start(over_p, k)
        start(over_z, k)

    each(piece, LAG)

    row_edge = jnp.where(both(odd, jnp.logical_not(has_z)), row_at, 0.0)
    column_edge = jnp.where(has_right, 0.0, column_at)

    def renew(k):
        arrive(over_p, k)
        arrive(over_z, k)
        rows, mates = ds(k), near_mate(k, own)
        inside = both(
            (iota(part, 0) + k * size).astype(F32) >= row_edge,
            count_up(part, 1) >= column_edge,
        )
        planes = [
            jnp.where(
                inside,
                win[p, rows] - step_size * jnp.where(mates, got_p[p, rows], got_z[p, rows]),
                0.0,
            )
            for p in range(2)
        ]
        step_in(k, planes)

    def exchange(k):
        when(k + LAG < CHUNKS, lambda: piece(k + LAG))
        spread(k)
        when(k >= BACK, lambda: renew(k - BACK))

    each(exchange)
    each(lambda k: renew(k + CHUNKS - BACK), BACK)
    each(middle, width // wide)

    def last_piece(k):
        rows = ds(k)
        grads = slope(k)
        for p in range(2):
            total[p, rows] = grad1[p, rows] + grads[p]
        start(last_right, k)

    def scatter(k):
        arrive(last_right, k)
        rows = ds(k)
        low, low_l, far, far_l = low_of(k, own), low_of(k, meta_l), far_of(own), far_of(meta_l)
        for p in range(2):
            mine = jnp.where(far, 0.0, total[p, rows])
            theirs = jnp.where(far_l, from_left2[p, rows], 0.0)
            mine_low, theirs_low = jnp.where(low, mine, 0.0), jnp.where(low_l, theirs, 0.0)
            lower = mine_low + theirs_low
            upper = (mine - mine_low) + (theirs - theirs_low)
            give_z2[p, rows] = lower
            give_y2[p, rows] = jnp.where(swapped, upper, lower)
            kept = jnp.where(swapped, jnp.where(odd, 0.0, lower), upper)
            out[p, rows] = spec[p, rows] - step_size * kept
        start(z_out, k)
        when(jnp.logical_not(both(swapped, even)), lambda: start(y_out, k))

    def pass_on(k):
        @pl.when(both(swapped, even))
        def _():
            arrive(z_out, k)
            rows = ds(k)
            for p in range(2):
                give_y2[p, rows] = give_y2[p, rows] + got_z2[p, rows]
            launch(y_out[0], k)

    def finale(k):
        when(stay, lambda: arrive(z_out, k))
        arrive(y_out, k)
        rows = ds(k)
        for p in range(2):
            came = jnp.where(either(swapped, odd), got_y2[p, rows], got_z2[p, rows])
            out[p, rows] = out[p, rows] - step_size * came

    each(last_piece, LAG)

    def first_scatter(k):
        last_piece(k + LAG)
        scatter(k)

    each(first_scatter, RELAY)

    def steady(k):
        last_piece(k + LAG + RELAY)
        scatter(k + RELAY)
        pass_on(k)

    each(steady, CHUNKS - LAG - RELAY)

    def drain(k):
        scatter(k + CHUNKS - LAG)
        pass_on(k + CHUNKS - LAG - RELAY)

    each(drain, LAG)
    each(lambda k: pass_on(k + CHUNKS - RELAY), RELAY)
    each(finale)

    when(swapped, meta_swap.wait_send)
    when(straight, amps_flow.wait_send)

    for copy, sends, _ in meta_flows:
        when(sends, copy.wait_send)

    def sent(k):
        for one in flows:
            when(one[1], lambda: one[0](k).wait_send())

    each(lambda k: sent(k + CHUNKS - DEPTH), DEPTH)


def on_device(n_row, n_col, spectrum, pupil, amplitudes, offsets, counts):
    width = pupil.shape[1]
    amps = amplitudes[0, 0, 0]
    place = offsets.reshape(-1)
    count = counts.reshape(-1)
    cosine, sine = dft_tables(width)
    plane = pltpu.VMEM((2, width, width), F32)
    table = pltpu.VMEM((2 * width, 2 * width), BF16)
    stage = pltpu.VMEM((2 * width, width), BF16)
    note = pltpu.VMEM((3, 8, width), F32)
    vmem = pl.BlockSpec(memory_space=pltpu.VMEM)
    return pl.pallas_call(
        functools.partial(kernel, n_row, n_col),
        out_shape=jax.ShapeDtypeStruct(spectrum.shape, F32),
        in_specs=[pl.BlockSpec(memory_space=pltpu.SMEM)] * 2
        + [vmem]
        + [pl.BlockSpec(memory_space=pltpu.MemorySpace.HBM)] * 4,
        out_specs=vmem,
        scratch_shapes=[plane] * 20
        + [table] * 4
        + [stage] * 2
        + [pltpu.VMEM((2, width, width), BF16)]
        + [note] * 6
        + [
            pltpu.SemaphoreType.DMA((15, CHUNKS)),
            pltpu.SemaphoreType.DMA((15, CHUNKS)),
            pltpu.SemaphoreType.DMA((5,)),
            pltpu.SemaphoreType.DMA((5,)),
            pltpu.SemaphoreType.DMA((2,)),
            pltpu.VMEM((width, width), F32),
            pltpu.VMEM((width, width), F32),
            plane,
            pltpu.VMEM((width, width), F32),
            pltpu.VMEM((width, width), BF16),
            pltpu.VMEM((width, width), BF16),
            pltpu.SemaphoreType.DMA((4,)),
        ],
        compiler_params=pltpu.CompilerParams(
            collective_id=0, has_side_effects=True, vmem_limit_bytes=67 * 1000 * 1000
        ),
    )(place, count, spectrum, pupil, amps, cosine, sine)


def solution(mesh):
    in_specs = (
        P(None, "row", "col"),
        P(),
        P("row", "col", None, None, None),
        P("row", "col", None, None),
        P("row", "col"),
    )
    return jax.shard_map(
        functools.partial(on_device, mesh.shape["row"], mesh.shape["col"]),
        mesh=mesh, in_specs=in_specs, out_specs=P(None, "row", "col"), check_vma=False,
    )
```

```python
import functools
import math

import jax
import jax.numpy as jnp
import numpy as np
from jax import lax
from jax.experimental import pallas as pl
from jax.experimental.pallas import tpu as pltpu
from jax.sharding import PartitionSpec as P

SWEEPS = 2
CHUNKS = 16
DEPTH = 2
LAG = 3
BACK = 3
RELAY = 2

step_size = 0.5
floor_value = 0.05

MESH = pl.DeviceIdType.MESH
BF16 = jnp.bfloat16
F32 = jnp.float32


def dft_tables(width):
    index = np.arange(width)
    angle = (index[:, None] * index[None, :] % width) * (2.0 * math.pi / width)
    scale = 1.0 / math.sqrt(width)
    return (
        jnp.asarray((np.cos(angle) * scale).astype(np.float32).astype(BF16)),
        jnp.asarray((np.sin(angle) * scale).astype(np.float32).astype(BF16)),
    )


def dot(a, b):
    return jnp.dot(a, b, preferred_element_type=F32)


def iota(shape, axis):
    return lax.broadcasted_iota(jnp.int32, shape, axis)


def kernel(
    n_row, n_col, place, count, spec_in, pupil_in, amps_in, cosine_in, sine_in, out_hbm,
    spec, out, spec_sem, out_sem,
    y1, z1, side1, mix1, win, grad1, from_left1, from_right1, give_p, got_p, give_z, got_z,
    total, from_left2, give_z2, got_z2, give_y2, got_y2,
    hop, pup, fwd_right, fwd_left, back_right, back_left, f1, f2, hot,
    here, own, meta_l, meta_r, meta_p, meta_z,
    send, recv, meta_send, meta_recv, amps_sem, first_amps, next_amps,
    pupil, amps, cosine, sine, load,
):
    width = spec.shape[1]
    size = width // CHUNKS
    r, c = lax.axis_index("row"), lax.axis_index("col")
    parity = lax.rem(r, 2)
    mate = r + 1 - 2 * parity
    swapped = lax.rem(r // 2, 2) == 1
    home = jnp.where(swapped, mate, r)
    odd = lax.rem(home, 2) == 1
    even = jnp.logical_not(odd)
    has_z = jnp.where(odd, home < n_row - 1, home > 0)
    has_left, has_right = c > 0, c < n_col - 1
    left = (r, lax.rem(c + n_col - 1, n_col))
    right = (r, lax.rem(c + 1, n_col))
    partner = (mate, c)
    beyond = (lax.rem(jnp.where(odd, r + 2, r + n_row - 2), n_row), c)
    has_cross = jnp.where(swapped, True, r + 2 < n_row)
    cross = (lax.rem(jnp.where(swapped, r + n_row - 2, r + 2), n_row), c)
    detour = lax.rem(c, 2) == 1
    always = r >= 0
    side = jnp.where(odd, -1.0, 1.0)

    def both(*conditions):
        return functools.reduce(jnp.logical_and, conditions)

    def either(*conditions):
        return functools.reduce(jnp.logical_or, conditions)

    def when(condition, body):
        if not isinstance(condition, bool):
            pl.when(condition)(body)
        elif condition:
            body()

    stay = jnp.logical_not(swapped)
    spec_load = pltpu.make_async_copy(spec_in, spec, spec_sem.at[0])
    spec_load.start()
    loads = [
        pltpu.make_async_copy(source, target, load.at[at])
        for at, (source, target) in enumerate(
            ((cosine_in, cosine), (sine_in, sine), (pupil_in, pupil))
        )
    ]
    for copy in loads:
        copy.start()
    own_amps = pltpu.make_async_copy(amps_in, amps, load.at[3])
    when(stay, own_amps.start)
    for at, value in enumerate((place[0].astype(F32), place[1].astype(F32), jnp.where(count[0] > 0, 1.0, 0.0))):
        here[at] = jnp.zeros(here.shape[1:], F32) + value

    def ds(k, block=size, base=0):
        return pl.ds(pl.multiple_of(base + k * block, 8), block)

    def flow(kind, src, dst, device):
        def copy(k):
            return pltpu.make_async_remote_copy(
                src_ref=src.at[:, ds(k), :], dst_ref=dst.at[:, ds(k), :],
                send_sem=send.at[kind, k], recv_sem=recv.at[kind, k],
                device_id=device, device_id_type=MESH,
            )
        return copy

    def flat(kind, src, dst, device):
        def copy(k):
            return pltpu.make_async_remote_copy(
                src_ref=src.at[ds(k), :], dst_ref=dst.at[ds(k), :],
                send_sem=send.at[kind, k], recv_sem=recv.at[kind, k],
                device_id=device, device_id_type=MESH,
            )
        return copy

    def each(body, count=CHUNKS):
        def step(k, carry):
            body(k)
            return carry
        lax.fori_loop(0, count, step, 0)

    neighbours = (
        (always, partner), (has_z, beyond), (has_left, left), (has_right, right),
        (both(parity == 0, has_cross), cross),
    )
    barrier = pltpu.get_barrier_semaphore()
    for there, device in neighbours:
        @pl.when(there)
        def _():
            pl.semaphore_signal(barrier, inc=1, device_id=device, device_id_type=MESH)
    pl.semaphore_wait(barrier, sum(there.astype(jnp.int32) for there, _ in neighbours))

    def meta_copy(at, src, dst, device):
        return pltpu.make_async_remote_copy(
            src_ref=src, dst_ref=dst, send_sem=meta_send.at[at], recv_sem=meta_recv.at[at],
            device_id=device, device_id_type=MESH,
        )

    meta_swap = meta_copy(0, here, own, partner)
    meta_flows = (
        (meta_copy(1, own, meta_r, left), has_left, has_right),
        (meta_copy(2, own, meta_l, right), has_right, has_left),
        (meta_copy(3, own, meta_p, partner), always, always),
        (meta_copy(4, own, meta_z, beyond), has_z, has_z),
    )

    y_in = (flow(0, spec, y1, partner), either(swapped, odd), either(swapped, even))
    direct = jnp.logical_not(detour)
    z_in = (
        flow(1, spec, z1, beyond), both(stay, even, has_z), both(odd, has_z, either(swapped, direct))
    )
    z_relay = (flow(1, y1, z1, beyond), both(swapped, even, has_z, direct), False)
    hop_in = (flow(10, spec, hop, cross), both(swapped, odd, detour), both(stay, even, has_cross, detour))
    z_hop = (flow(11, hop, z1, partner), both(stay, even, has_cross, detour), both(stay, odd, has_z, detour))
    relays_amps = both(stay, detour, has_cross)
    amps_1 = (flat(12, amps_in, first_amps, cross), both(swapped, detour), relays_amps)
    amps_2 = (flat(13, first_amps, next_amps, partner), relays_amps, relays_amps)
    amps_3 = (flat(14, next_amps, amps, cross), relays_amps, both(swapped, detour))
    straight = both(swapped, direct)
    amps_flow = pltpu.make_async_remote_copy(
        src_ref=amps_in, dst_ref=amps, send_sem=amps_sem.at[0], recv_sem=amps_sem.at[1],
        device_id=partner, device_id_type=MESH,
    )
    mix_in = (flow(2, mix1, side1, left), has_left, has_right)
    grad_right = (flow(3, grad1, from_left1, right), has_right, has_left)
    grad_left = (flow(4, grad1, from_right1, left), has_left, has_right)
    over_p = (flow(5, give_p, got_p, partner), always, always)
    over_z = (flow(6, give_z, got_z, beyond), has_z, has_z)
    last_right = (flow(7, total, from_left2, right), has_right, has_left)
    z_out = (flow(8, give_z2, got_z2, beyond), both(odd, has_z), both(even, has_z))
    y_out = (flow(9, give_y2, got_y2, partner), either(swapped, even), either(swapped, odd))
    flows = (y_in, z_in, mix_in, grad_right, grad_left, over_p, over_z, last_right, z_out, y_out,
             z_relay, hop_in, z_hop, amps_1, amps_2, amps_3)

    def launch(copy, k):
        when(k >= DEPTH, lambda: copy(k - DEPTH).wait_send())
        copy(k).start()

    def start(one, k):
        when(one[1], lambda: launch(one[0], k))

    def arrive(one, k):
        when(one[2], lambda: one[0](k).wait_recv())

    when(swapped, meta_swap.start)

    def first_sends(k):
        for one in (y_in, z_in, hop_in):
            start(one, k)

    spec_load.wait()
    for k in range(DEPTH):
        first_sends(k)
    for k in range(DEPTH):
        start(amps_1, k)

    @pl.when(stay)
    def _():
        own[...] = here[...]

    def clear(*refs):
        for ref in refs:
            ref[...] = jnp.zeros_like(ref)

    when(jnp.logical_not(has_left), lambda: clear(from_left1, from_left2, meta_l))
    when(jnp.logical_not(has_right), lambda: clear(side1, from_right1, meta_r))
    when(jnp.logical_not(has_z), lambda: clear(z1, got_z, got_z2, meta_z))
    when(swapped, meta_swap.wait_recv)
    for copy, sends, _ in meta_flows:
        when(sends, copy.start)

    row_at, column_at, live = own[0, 0:1, :], own[1, 0:1, :], own[2, 0:1, :]

    def count_up(shape, axis):
        return iota(shape, axis).astype(F32)

    part = (size, width)

    def low_of(k, ref):
        return (iota(part, 0) + k * size).astype(F32) < ref[0, 0:1, :]

    def near_mate(k, ref):
        return side * ((iota(part, 0) + k * size).astype(F32) - ref[0, 0:1, :] + 0.5) < 0.0

    def far_of(ref):
        return count_up(part, 1) < ref[1, 0:1, :]

    def tiles(k, p):
        rows = ds(k)
        near = jnp.where(swapped, y1[p, rows], spec[p, rows])
        mine = jnp.where(swapped, spec[p, rows], y1[p, rows])
        return near, jnp.where(odd, z1[p, rows], mine)

    def relay(k):
        arrive(y_in, k)
        start(z_relay, k)
        arrive(hop_in, k)
        start(z_hop, k)
        when(k + DEPTH < CHUNKS, lambda: first_sends(k + DEPTH))

    def mix(k):
        arrive(z_in, k)
        arrive(z_hop, k)
        rows = ds(k)
        own_low, left_low = low_of(k, own), low_of(k, meta_l)
        for p in range(2):
            near, below = tiles(k, p)
            win[p, rows] = jnp.where(own_low, below, near)
            mix1[p, rows] = jnp.where(left_low, below, near)
        start(mix_in, k)

    for copy, _, receives in meta_flows:
        when(receives, copy.wait_recv)

    def second(k):
        arrive(amps_1, k)
        start(amps_2, k)

    def third(k):
        arrive(amps_2, k)
        start(amps_3, k)

    def ahead(k):
        when(k + 2 < CHUNKS, lambda: relay(k + 2))
        mix(k)
        when(k + 4 < CHUNKS, lambda: start(amps_1, k + 4))
        when(k + 2 < CHUNKS, lambda: second(k + 2))
        third(k)
        when(k == CHUNKS - 5, lambda: when(straight, amps_flow.start))

    block = 128
    shape = (block, width)

    def wrapped(value):
        return jnp.where(value >= width, value - width, value)

    def one_hot(mask):
        return jnp.where(mask, 1.0, 0.0).astype(BF16)

    def columns_of(i):
        at = (iota(shape, 0) + i * block).astype(F32)
        hot[0, ds(i, block)] = one_hot(count_up(shape, 1) == wrapped(at + row_at))
        hot[1, ds(i, block)] = one_hot(count_up(shape, 1) == wrapped(at + column_at))

    each(columns_of, width // block)
    relay(0)
    relay(1)
    for k in range(DEPTH, 4):
        start(amps_1, k)
    second(0)
    second(1)
    ahead(0)

    def rows_hot(i, shift):
        at = (iota(shape, 0) + i * block).astype(F32)
        return one_hot(at == wrapped(count_up(shape, 1) + shift))

    def tables(i):
        top, low = ds(i, block), ds(i, block, width)
        near, far = pl.ds(0, width), pl.ds(width, width)

        def put(ref, cos, sin, top_sign, low_sign):
            ref[top, near] = cos.astype(BF16)
            ref[low, far] = cos.astype(BF16)
            ref[top, far] = (top_sign * sin).astype(BF16)
            ref[low, near] = (low_sign * sin).astype(BF16)

        hot_rows = rows_hot(i, column_at)
        put(fwd_right, dot(hot_rows, cosine[...]), dot(hot_rows, sine[...]), 1.0, -1.0)
        hot_rows = rows_hot(i, row_at)
        put(back_left, dot(hot_rows, cosine[...]), dot(hot_rows, sine[...]), 1.0, -1.0)
        cos, sin = cosine[ds(i, block)], sine[ds(i, block)]
        put(fwd_left, dot(cos, hot[0]), dot(sin, hot[0]), -1.0, 1.0)
        put(back_right, dot(cos, hot[1]), dot(sin, hot[1]), -1.0, 1.0)

    for copy in loads:
        copy.wait()

    def beside(body, first, every):
        blocks = width // block

        def step(i):
            body(i)
            when(lax.rem(i, every) == every - 1, lambda: ahead(first + i // every))

        each(step, blocks)
        return first + blocks // every

    at = beside(tables, 1, 2)

    def three(value):
        high = value.astype(BF16)
        rest = value - high.astype(F32)
        middle = rest.astype(BF16)
        return high, middle, (rest - middle.astype(F32)).astype(BF16)

    for plane in range(2):
        def pupil_columns(i):
            parts = three(pupil[plane, ds(i, block)])
            moved = [dot(part, hot[1]) for part in parts]
            f1[ds(i, block)] = moved[0].astype(BF16)
            f1[ds(i, block, width)] = moved[1].astype(BF16)
            f2[ds(i, block)] = moved[2].astype(BF16)

        at = beside(pupil_columns, at, 4)

        def pupil_rows(i):
            hot_rows = rows_hot(i, row_at)
            high = dot(hot_rows, f1[0:width])
            middle = dot(hot_rows, f1[width : 2 * width])
            pup[plane, ds(i, block)] = high + middle + dot(hot_rows, f2[0:width])

        at = beside(pupil_rows, at, 4)

    def step_in(k, planes):
        rows = ds(k)
        pr, pi = pup[0, rows], pup[1, rows]
        field_real = planes[0] * pr - planes[1] * pi
        field_imag = planes[0] * pi + planes[1] * pr
        joined = jnp.concatenate([field_real, field_imag], axis=1).astype(BF16)
        first = dot(joined, fwd_right[...])
        f1[rows] = first[:, :width].astype(BF16)
        f1[ds(k, size, width)] = first[:, width:].astype(BF16)

    def consume(k):
        arrive(mix_in, k)
        rows, far = ds(k), far_of(own)
        planes = [jnp.where(far, side1[p, rows], win[p, rows]) for p in range(2)]
        for p in range(2):
            win[p, rows] = planes[p]
        step_in(k, planes)

    late = CHUNKS - at
    pairs = (CHUNKS - 2) - late

    def catch_up(k):
        ahead(at + k)
        consume(2 * k)
        consume(2 * k + 1)

    def keep_up(k):
        ahead(at + pairs + k)
        consume(2 * pairs + k)

    each(catch_up, pairs)
    each(keep_up, late - pairs)
    each(lambda k: consume(CHUNKS - 2 + k), 2)

    wide = width // 2

    def wave_of(i):
        rows, low = ds(i, wide), ds(i, wide, width)
        wave = dot(jnp.concatenate([fwd_left[rows], fwd_left[low]], axis=0), f1[...])
        return wave[:wide], wave[wide:]

    def misfit(i, wave_real, wave_imag):
        rows, low = ds(i, wide), ds(i, wide, width)
        magnitude = jnp.sqrt(wave_real * wave_real + wave_imag * wave_imag)
        keep = 1.0 - amps[rows] / jnp.maximum(magnitude, floor_value)
        joined = jnp.concatenate([wave_real * keep, wave_imag * keep], axis=1).astype(BF16)
        first = dot(joined, back_right[...])
        f2[rows] = first[:, :width].astype(BF16)
        f2[low] = first[:, width:].astype(BF16)

    def middle(i):
        misfit(i, *wave_of(i))

    def early_wave(i):
        rows = ds(i, wide)
        give_y2[0, rows], give_y2[1, rows] = wave_of(i)

    def late_misfit(i):
        rows = ds(i, wide)
        misfit(i, give_y2[0, rows], give_y2[1, rows])

    def slope(k):
        rows, low = ds(k), ds(k, size, width)
        back = dot(jnp.concatenate([back_left[rows], back_left[low]], axis=0), f2[...])
        back_real, back_imag = back[:size], back[size:]
        pr, pi = pup[0, rows], pup[1, rows]
        return (
            (back_real * pr + back_imag * pi) * live,
            (back_imag * pr - back_real * pi) * live,
        )

    each(early_wave, width // wide)
    when(stay, own_amps.wait)
    each(lambda k: arrive(amps_3, k))
    when(straight, amps_flow.wait_recv)
    each(late_misfit, width // wide)

    def piece(k):
        rows = ds(k)
        grads = slope(k)
        for p in range(2):
            grad1[p, rows] = grads[p]
        start(grad_right, k)
        start(grad_left, k)

    def spread(k):
        arrive(grad_right, k)
        arrive(grad_left, k)
        rows = ds(k)
        mates, mates_l, mates_r = near_mate(k, own), near_mate(k, meta_l), near_mate(k, meta_r)
        far, far_l, far_r = far_of(own), far_of(meta_l), far_of(meta_r)
        far_p, far_z = far_of(meta_p), far_of(meta_z)
        for p in range(2):
            mine = grad1[p, rows]
            mine_near, mine_far = jnp.where(far, 0.0, mine), jnp.where(far, mine, 0.0)
            near = jnp.where(far_l, from_left1[p, rows], 0.0)
            past = jnp.where(far_r, 0.0, from_right1[p, rows])
            near_p, past_p = jnp.where(mates_l, near, 0.0), jnp.where(mates_r, past, 0.0)
            near_z, past_z = near - near_p, past - past_p
            give_p[p, rows] = jnp.where(
                far_p,
                jnp.where(mates, mine_far, 0.0) + past_p,
                jnp.where(mates, mine_near, 0.0) + near_p,
            )
            give_z[p, rows] = jnp.where(
                far_z,
                jnp.where(mates, 0.0, mine_far) + past_z,
                jnp.where(mates, 0.0, mine_near) + near_z,
            )
            beside = jnp.where(
                far, jnp.where(mates, past_p, past_z), jnp.where(mates, near_p, near_z)
            )
            win[p, rows] = win[p, rows] - step_size * (mine + beside)
        start(over_p, k)
        start(over_z, k)

    each(piece, LAG)

    row_edge = jnp.where(both(odd, jnp.logical_not(has_z)), row_at, 0.0)
    column_edge = jnp.where(has_right, 0.0, column_at)

    def renew(k):
        arrive(over_p, k)
        arrive(over_z, k)
        rows, mates = ds(k), near_mate(k, own)
        inside = both(
            (iota(part, 0) + k * size).astype(F32) >= row_edge,
            count_up(part, 1) >= column_edge,
        )
        planes = [
            jnp.where(
                inside,
                win[p, rows] - step_size * jnp.where(mates, got_p[p, rows], got_z[p, rows]),
                0.0,
            )
            for p in range(2)
        ]
        step_in(k, planes)

    def exchange(k):
        when(k + LAG < CHUNKS, lambda: piece(k + LAG))
        spread(k)
        when(k >= BACK, lambda: renew(k - BACK))

    each(exchange)
    each(lambda k: renew(k + CHUNKS - BACK), BACK)
    each(middle, width // wide)

    def last_piece(k):
        rows = ds(k)
        grads = slope(k)
        for p in range(2):
            total[p, rows] = grad1[p, rows] + grads[p]
        start(last_right, k)

    def scatter(k):
        arrive(last_right, k)
        rows = ds(k)
        low, low_l, far, far_l = low_of(k, own), low_of(k, meta_l), far_of(own), far_of(meta_l)
        for p in range(2):
            mine = jnp.where(far, 0.0, total[p, rows])
            theirs = jnp.where(far_l, from_left2[p, rows], 0.0)
            mine_low, theirs_low = jnp.where(low, mine, 0.0), jnp.where(low_l, theirs, 0.0)
            lower = mine_low + theirs_low
            upper = (mine - mine_low) + (theirs - theirs_low)
            give_z2[p, rows] = lower
            give_y2[p, rows] = jnp.where(swapped, upper, lower)
            kept = jnp.where(swapped, jnp.where(odd, 0.0, lower), upper)
            out[p, rows] = spec[p, rows] - step_size * kept
        start(z_out, k)
        when(jnp.logical_not(both(swapped, even)), lambda: start(y_out, k))

    def pass_on(k):
        @pl.when(both(swapped, even))
        def _():
            arrive(z_out, k)
            rows = ds(k)
            for p in range(2):
                give_y2[p, rows] = give_y2[p, rows] + got_z2[p, rows]
            launch(y_out[0], k)

    def stored(k):
        return pltpu.make_async_copy(
            out.at[:, ds(k), :], out_hbm.at[:, ds(k), :], out_sem.at[k]
        )

    def finale(k):
        when(stay, lambda: arrive(z_out, k))
        arrive(y_out, k)
        rows = ds(k)
        for p in range(2):
            came = jnp.where(either(swapped, odd), got_y2[p, rows], got_z2[p, rows])
            out[p, rows] = out[p, rows] - step_size * came
        stored(k).start()

    each(last_piece, LAG)

    def first_scatter(k):
        last_piece(k + LAG)
        scatter(k)

    each(first_scatter, RELAY)

    def steady(k):
        last_piece(k + LAG + RELAY)
        scatter(k + RELAY)
        pass_on(k)

    each(steady, CHUNKS - LAG - RELAY)

    def drain(k):
        scatter(k + CHUNKS - LAG)
        pass_on(k + CHUNKS - LAG - RELAY)

    each(drain, LAG)
    each(lambda k: pass_on(k + CHUNKS - RELAY), RELAY)
    each(finale)

    each(lambda k: stored(k).wait())
    when(swapped, meta_swap.wait_send)
    when(straight, amps_flow.wait_send)

    for copy, sends, _ in meta_flows:
        when(sends, copy.wait_send)

    def sent(k):
        for one in flows:
            when(one[1], lambda: one[0](k).wait_send())

    each(lambda k: sent(k + CHUNKS - DEPTH), DEPTH)


def on_device(n_row, n_col, spectrum, pupil, amplitudes, offsets, counts):
    width = pupil.shape[1]
    amps = amplitudes[0, 0, 0]
    place = offsets.reshape(-1)
    count = counts.reshape(-1)
    cosine, sine = dft_tables(width)
    plane = pltpu.VMEM((2, width, width), F32)
    table = pltpu.VMEM((2 * width, 2 * width), BF16)
    stage = pltpu.VMEM((2 * width, width), BF16)
    note = pltpu.VMEM((3, 8, width), F32)
    hbm = pl.BlockSpec(memory_space=pltpu.MemorySpace.HBM)
    return pl.pallas_call(
        functools.partial(kernel, n_row, n_col),
        out_shape=jax.ShapeDtypeStruct(spectrum.shape, F32),
        in_specs=[pl.BlockSpec(memory_space=pltpu.SMEM)] * 2 + [hbm] * 5,
        out_specs=hbm,
        scratch_shapes=[plane] * 2
        + [pltpu.SemaphoreType.DMA((1,)), pltpu.SemaphoreType.DMA((CHUNKS,))]
        + [plane] * 20
        + [table] * 4
        + [stage] * 2
        + [pltpu.VMEM((2, width, width), BF16)]
        + [note] * 6
        + [
            pltpu.SemaphoreType.DMA((15, CHUNKS)),
            pltpu.SemaphoreType.DMA((15, CHUNKS)),
            pltpu.SemaphoreType.DMA((5,)),
            pltpu.SemaphoreType.DMA((5,)),
            pltpu.SemaphoreType.DMA((2,)),
            pltpu.VMEM((width, width), F32),
            pltpu.VMEM((width, width), F32),
            plane,
            pltpu.VMEM((width, width), F32),
            pltpu.VMEM((width, width), BF16),
            pltpu.VMEM((width, width), BF16),
            pltpu.SemaphoreType.DMA((4,)),
        ],
        compiler_params=pltpu.CompilerParams(
            collective_id=0, has_side_effects=True, vmem_limit_bytes=67 * 1000 * 1000
        ),
    )(place, count, spectrum, pupil, amps, cosine, sine)


def solution(mesh):
    in_specs = (
        P(None, "row", "col"),
        P(),
        P("row", "col", None, None, None),
        P("row", "col", None, None),
        P("row", "col"),
    )
    return jax.shard_map(
        functools.partial(on_device, mesh.shape["row"], mesh.shape["col"]),
        mesh=mesh, in_specs=in_specs, out_specs=P(None, "row", "col"), check_vma=False,
    )
```
